256 devices in a mesh: band: 4 (over y, x), row: 64 (over z, core).
Axes of the slice: x: 2, y: 2, z: 32, core: 2. Of those that a mesh axis runs over, the one named last changes fastest.
The devices are a block of a 4x8x32 slice.
Arguments:
- shot_traces: bfloat16 [131072, 4096], P(('band', 'row')), parts along dimension 0, may hold values from -6 to 6
- source_cell: int32 [131072], P(('band', 'row')), parts along dimension 0, may hold values from 0 to 127
- receiver_cell: int32 [131072], P(('band', 'row')), parts along dimension 0, may hold values from 0 to 127
- band_order: int32 [512], P('band'), parts along dimension 0, may hold values from 0 to 127, each once
Outputs:
- next_grid: float32 [512, 2, 128, 128], P(('band', 'row')), parts along dimension 0
The draws below stay inside these ranges and needn't reach their ends.
There are 4 independent parts, one for each index of `band`. The reference program is written for one: setup_inputs(seed, part) draws one part's arguments, and reference() takes and returns one part's arrays. A program takes and returns all parts, laid end to end along the dimension named above; each array names one. Nothing has to cross between parts.
Inputs may be any that keep to these rules, and one draw needn't show every extreme that they name: `band_order`: a permutation of 0 to 127.
All inputs are finite; a program needn't handle non-finite values.
Results may differ from the reference program's by a relative error of at most 0.0037.
Values may be sent and summed in bfloat16 or wider, within the bound.
A program may use at most 64 MiB of HBM per device.

```python
import math
import jax
import jax.numpy as jnp
from jax import lax

NT = 4096
FLO = 64
SC = 128
RC = 128
NFB = 128
TRACES = 32768


def place_ends(drawn, stream_key, smallest, top_value):
    dims = drawn.shape
    index_at = [jax.random.randint(jax.random.fold_in(stream_key, axis), (), 0, dims[axis]) for axis in range(len(dims))]
    drawn = drawn.at[tuple(index_at)].set(smallest)
    longest = dims.index(max(dims))
    index_at[longest] = (index_at[longest] + 1) % dims[longest]
    return drawn.at[tuple(index_at)].set(top_value)


def shard_levels(rng, shape, split, smallest, top_value):
    def one(axis_at, shards_of):
        heights = jax.random.uniform(jax.random.fold_in(jax.random.fold_in(rng, 6), axis_at), (shards_of,), jnp.float32, smallest / len(split), top_value / len(split))
        return jnp.repeat(jnp.exp(heights), shape[axis_at] // shards_of).reshape((-1,) + (1,) * (len(shape) - axis_at - 1))

    loudness = one(*split[0])
    for cut in split[1:]:
        loudness = loudness * one(*cut)
    return loudness


def gaussian(own_key, extent, scale, limit, shards=(), held_as=jnp.bfloat16):
    result = jax.random.normal(own_key, extent, jnp.float32) * scale
    if len(shards) > 0:
        result = shard_levels(own_key, extent, shards, -0.22, 0.18) * result
    return jnp.clip(result, min=-limit, max=limit).astype(held_as)


def setup_inputs(seed: int = 0, part: int = 0) -> dict:
    streams_of = jax.random.split(jax.random.key(seed), 5)
    part_splits = jax.random.split(jax.random.fold_in(streams_of[4], part), 5)
    shot_traces = gaussian(part_splits[0], (TRACES, NT), 1.0, 6.0, ((0, 64),))
    source_cell = place_ends(jax.random.randint(part_splits[1], (TRACES,), 0, SC), jax.random.fold_in(part_splits[1], 1), 0, SC - 1).astype(jnp.int32)
    receiver_cell = place_ends(jax.random.randint(part_splits[2], (TRACES,), 0, RC), jax.random.fold_in(part_splits[2], 1), 0, RC - 1).astype(jnp.int32)
    band_order = jax.random.permutation(part_splits[3], NFB).astype(jnp.int32)
    return dict(shot_traces=shot_traces, source_cell=source_cell, receiver_cell=receiver_cell, band_order=band_order)


def reference(shot_traces, source_cell, receiver_cell, band_order):
    high = lax.Precision.HIGHEST
    bins = (FLO + band_order).astype(jnp.int32)
    samples = jnp.arange(NT, dtype=jnp.int32)
    phase = samples[:, None] * bins[None, :] % NT
    angle = 2.0 * math.pi * phase.astype(jnp.float32) / NT
    scale = 1.0 / math.sqrt(NT)
    table = jnp.concatenate([jnp.cos(angle) * scale, -jnp.sin(angle) * scale], axis=1).astype(jnp.bfloat16)
    spectra = jnp.dot(shot_traces.astype(jnp.float32), table.astype(jnp.float32), precision=high).astype(jnp.bfloat16)
    cell_ids = (source_cell * RC + receiver_cell).astype(jnp.int32)
    stack = jax.ops.segment_sum(spectra.astype(jnp.float32), cell_ids, num_segments=SC * RC)
    counts = jax.ops.segment_sum(jnp.ones(cell_ids.shape, jnp.float32), cell_ids, num_segments=SC * RC)
    stack = stack.reshape(SC, RC, 2, NFB).transpose(3, 2, 0, 1)
    next_grid = stack / jnp.maximum(counts.reshape(SC, RC), 1.0)[None, None, :, :]
    return next_grid
```

```python
import functools
import math

import jax
import jax.numpy as jnp
import numpy as np
from jax import lax
from jax.experimental import pallas as pl
from jax.experimental.pallas import tpu as pltpu
from jax.sharding import PartitionSpec as P

FLO = 64
SC = 128
RC = 128
MESH = pl.DeviceIdType.MESH
NT_DIMS = (((1,), (1,)), ((), ()))
CHUNKS = 4
STRIDE = 4
SELF = 31
FAR = 30


def twiddles(samples, band):
    bins = FLO + np.arange(band, dtype=np.int64)
    phase = (np.arange(samples, dtype=np.int64)[:, None] * bins[None, :]) % samples
    angle = (2.0 * math.pi * phase.astype(np.float32) / samples).astype(np.float32)
    scale = 1.0 / math.sqrt(samples)
    table = np.concatenate([np.cos(angle) * scale, -np.sin(angle) * scale], axis=1)
    return jnp.asarray(table.astype(np.float32)).astype(jnp.bfloat16)


def final_base(level, side):
    return 24 + 4 * (2 * (level - 1) + side)


def transit_base(level, hop, side):
    if hop == level:
        return final_base(level, side)
    return 48 + 4 * (2 * {(2, 1): 0, (3, 1): 1, (3, 2): 2}[(level, hop)] + side)


FAR_BASE = 72
SLOTS = 76


def leg_cell(level, side):
    return 24 + 2 * (level - 1) + side


def kernel(
    chips,
    traces_hbm,
    table_hbm,
    source_ref,
    receiver_ref,
    order_ref,
    stack_ref,
    counts_ref,
    traces,
    table,
    acc,
    staged,
    own,
    give,
    slots,
    cells,
    total,
    load_sem,
    send_sem,
    recv_sem,
):
    me = lax.axis_index("row")
    z = me // 2
    core = me % 2
    band = order_ref.shape[1]
    samples = traces.shape[1]
    part = samples // CHUNKS

    def peer(step):
        return {"row": ((z + step + chips) % chips) * 2 + core}

    partner = {"row": z * 2 + (1 - core)}
    towards = (1, -1)
    far_way = 1 - 2 * core

    loads = []
    for k in range(CHUNKS):
        span = pl.ds(k * part, part)
        loads.append(
            (
                pltpu.make_async_copy(table_hbm.at[span, :], table.at[span, :], load_sem.at[2 * k]),
                pltpu.make_async_copy(
                    traces_hbm.at[:, span], traces.at[:, span], load_sem.at[2 * k + 1]
                ),
            )
        )
    for pair in loads:
        for copy in pair:
            copy.start()

    barrier = pltpu.get_barrier_semaphore()
    greeted = [partner] + [peer(way * step) for step in range(1, STRIDE + 1) for way in towards]
    for who in greeted:
        pl.semaphore_signal(barrier, inc=1, device_id=who, device_id_type=MESH)

    source = source_ref[...]
    cells[SELF, 0, 0:4, :] = (source // 2).astype(jnp.float32).astype(jnp.bfloat16)
    cells[SELF, 0, 4:8, :] = (
        ((source % 2) * RC + receiver_ref[...]).astype(jnp.float32).astype(jnp.bfloat16)
    )
    total[...] = jnp.zeros_like(total)

    row = lax.broadcasted_iota(jnp.int32, (band, band), 0)
    col = lax.broadcasted_iota(jnp.int32, (band, band), 1)
    wanted = 4 * ((z + row % 32) % chips) + 2 * ((core + (row // 32) % 2) % 2) + row // 64
    place = (wanted == col).astype(jnp.float32).astype(jnp.bfloat16)
    holds = (row == jnp.broadcast_to(order_ref[...], (band, band))).astype(jnp.float32)
    pick = lax.dot_general(
        place, holds.astype(jnp.bfloat16), NT_DIMS, preferred_element_type=jnp.float32
    ).astype(jnp.bfloat16)

    for k in range(CHUNKS):
        span = pl.ds(k * part, part)
        for copy in loads[k]:
            copy.wait()
        piece = jnp.dot(traces[:, span], table[span, :], preferred_element_type=jnp.float32)
        if k == 0:
            acc[...] = piece
        else:
            acc[...] += piece
    for c in range(2):
        half = acc[:, c * band : (c + 1) * band].astype(jnp.bfloat16)
        turned = lax.dot_general(pick, half, NT_DIMS, preferred_element_type=jnp.float32)
        for f in range(2):
            for x in range(2):
                for b in range(4):
                    staged[pl.ds(x * 512 + b * 4 + c * 2 + f, 32, stride=16), :] = turned[
                        f * 64 + x * 32 : f * 64 + x * 32 + 32, b * 128 : (b + 1) * 128
                    ]
    own[:, 0, :, :] = staged[0:512, :].reshape(32, 16, 128).astype(jnp.bfloat16)
    give[...] = staged[512:1024, :].reshape(32, 16, 128).astype(jnp.bfloat16)

    pl.semaphore_wait(barrier, len(greeted))

    started = []

    def send(src, dst, who):
        n = len(started)
        copy = pltpu.make_async_remote_copy(
            src_ref=src,
            dst_ref=dst,
            send_sem=send_sem.at[n],
            recv_sem=recv_sem.at[n],
            device_id=who,
            device_id_type=MESH,
        )
        copy.start()
        started.append(copy)
        return copy

    def swap_cells(first, count):
        return send(cells.at[pl.ds(first, count), 0], cells.at[pl.ds(first, count), 1], partner)

    def send_cells(src, level):
        out = []
        for step in range(1, 4):
            for side in range(2):
                out.append(
                    send(
                        cells.at[src[side], 0],
                        cells.at[6 * level + 3 * side + step - 1, 0],
                        peer(towards[side] * step),
                    )
                )
        return out

    leg = {}
    near_cells = {}
    swaps = {}
    leg[1] = [send(cells.at[SELF, 0], cells.at[leg_cell(1, s), 0], peer(4 * towards[s])) for s in range(2)]
    swaps["self"] = swap_cells(SELF, 1)
    swap_data = send(give, own.at[:, 1], partner)

    def sources(level, side):
        return 4 * level if side == 0 else 32 - 4 * level - 3

    hops = {}
    for lane in range(2):
        if lane == 1:
            swap_data.wait_recv()
        hops["far", 1, lane] = send(own.at[16, lane], slots.at[FAR_BASE, lane], peer(4 * far_way))
        for s in range(2):
            base = transit_base(3, 1, s)
            hops[3, 1, s, lane] = send(
                own.at[pl.ds(sources(3, s), 4), lane],
                slots.at[pl.ds(base, 4), lane],
                peer(4 * towards[s]),
            )
    near_cells[0] = send_cells((SELF, SELF), 0)
    for level in (2, 1):
        for s in range(2):
            base = transit_base(level, 1, s)
            hops[level, 1, s] = send(
                own.at[pl.ds(sources(level, s), 4)], slots.at[pl.ds(base, 4)], peer(4 * towards[s])
            )
    near = {0: []}
    for step in range(1, 4):
        for s in range(2):
            index = step if s == 0 else 32 - step
            near[0].append(
                send(own.at[index], slots.at[3 * s + step - 1], peer(towards[s] * step))
            )

    line = lax.broadcasted_iota(jnp.int32, (16, 128), 0).astype(jnp.float32)
    lines = [(line + 16.0 * g).astype(jnp.bfloat16) for g in range(16)]
    one = jnp.ones((16, 128), jnp.bfloat16)
    none = jnp.zeros((16, 128), jnp.bfloat16)

    def spread(rows, n):
        return jnp.broadcast_to(rows[n : n + 1, :], (16, 128)).astype(jnp.bfloat16)

    def binned(block, at, where):
        result = None
        for lane in range(2):
            value = block[at, lane].astype(jnp.float32)
            cell = cells[where, lane].astype(jnp.float32)
            for pair in range(2):
                left, right = [], []
                for b in (2 * pair, 2 * pair + 1):
                    high = spread(cell, b)
                    low = spread(cell, 4 + b)
                    hit = [high == lines[g] for g in range(4)]
                    rows = []
                    for cf in range(4):
                        v = spread(value, b * 4 + cf)
                        rows += [jnp.where(h, v, none) for h in hit]
                    rows += [jnp.where(h, one, none) for h in hit]
                    left.append(jnp.concatenate(rows, axis=0))
                    right.append(
                        jnp.concatenate([jnp.where(low == g, one, none) for g in lines], axis=0)
                    )
                piece = lax.dot_general(
                    jnp.concatenate(left, axis=1),
                    jnp.concatenate(right, axis=1),
                    NT_DIMS,
                    preferred_element_type=jnp.float32,
                )
                result = piece if result is None else result + piece
        total[...] += result

    def bin_many(first, pace, count, cell):
        def body(n, carry):
            binned(slots, first + pace * n, cell + n)
            return carry

        lax.fori_loop(0, count, body, 0)

    def wait_all(copies):
        for copy in copies:
            copy.wait_recv()

    def cells_step(level):
        wait_all(leg[level])
        if level < 3:
            leg[level + 1] = [
                send(cells.at[leg_cell(level, s), 0], cells.at[leg_cell(level + 1, s), 0], peer(4 * towards[s]))
                for s in range(2)
            ]
        else:
            leg[4] = [send(cells.at[leg_cell(3, 0) + core, 0], cells.at[FAR, 0], peer(4 * far_way))]
        near_cells[level] = send_cells((leg_cell(level, 0), leg_cell(level, 1)), level)
        swaps["leg", level] = swap_cells(leg_cell(level, 0), 2)

    def near_swap(level):
        wait_all(near_cells[level])
        swaps["near", level] = swap_cells(6 * level, 6)

    def onward(level, hop):
        for s in range(2):
            hops[level, hop, s].wait_recv()
            hops[level, hop + 1, s] = send(
                slots.at[pl.ds(transit_base(level, hop, s), 4)],
                slots.at[pl.ds(transit_base(level, hop + 1, s), 4)],
                peer(4 * towards[s]),
            )

    def far_onward(hop):
        if hop > 1:
            hops["far", hop].wait_recv()
        hops["far", hop + 1] = send(
            slots.at[FAR_BASE + hop - 1], slots.at[FAR_BASE + hop], peer(4 * far_way)
        )

    def deliver(level):
        for s in range(2):
            hops[level, level, s].wait_recv()
        near[level] = []
        for step in (3, 2, 1):
            for s in range(2):
                base = final_base(level, s)
                near[level].append(
                    send(
                        slots.at[base + (step if s == 0 else 3 - step)],
                        slots.at[6 * level + 3 * s + step - 1],
                        peer(towards[s] * step),
                    )
                )

    def bin_legs(level):
        swaps["leg", level].wait_recv()
        bin_many(final_base(level, 0), 7, 2, leg_cell(level, 0))

    def bin_near(level):
        wait_all(near[level])
        swaps["near", level].wait_recv()
        bin_many(6 * level, 1, 6, 6 * level)

    swaps["self"].wait_recv()
    binned(own, 0, SELF)
    cells_step(1)
    for lane in range(2):
        hops["far", 1, lane].wait_recv()
    far_onward(1)
    for s in range(2):
        hops[3, 1, s, 0].wait_recv()
        hops[3, 1, s] = hops[3, 1, s, 1]
    onward(3, 1)
    near_swap(0)
    onward(2, 1)
    cells_step(2)
    bin_near(0)
    near_swap(1)
    deliver(1)
    bin_legs(1)
    far_onward(2)
    onward(3, 2)
    cells_step(3)
    bin_near(1)
    near_swap(2)
    deliver(2)
    bin_legs(2)
    far_onward(3)
    wait_all(leg[4])
    swaps["far"] = swap_cells(FAR, 1)
    near_swap(3)
    bin_near(2)
    deliver(3)
    bin_legs(3)
    hops["far", 4].wait_recv()
    swaps["far"].wait_recv()
    bin_many(FAR_BASE + 3, 1, 1, FAR)
    bin_near(3)

    for cf in range(4):
        for odd in range(2):
            stack_ref[cf % 2, cf // 2, pl.ds(odd, 64, stride=2), :] = total[
                cf * 64 : cf * 64 + 64, odd * 128 : odd * 128 + 128
            ]
    for odd in range(2):
        counts_ref[pl.ds(odd, 64, stride=2), :] = total[256:320, odd * 128 : odd * 128 + 128]
    for copy in started:
        copy.wait_send()


COPIES = 100


def solution(mesh):
    rows = mesh.shape["row"]

    def local(shot_traces, source_cell, receiver_cell, band_order):
        count, samples = shot_traces.shape
        band = band_order.shape[0]
        per = band // rows
        vmem = pl.BlockSpec(memory_space=pltpu.VMEM)
        anywhere = pl.BlockSpec(memory_space=pl.ANY)
        stack, counts = pl.pallas_call(
            functools.partial(kernel, rows // 2),
            out_shape=(
                jax.ShapeDtypeStruct((per, 2, SC, RC), jnp.float32),
                jax.ShapeDtypeStruct((SC, RC), jnp.float32),
            ),
            in_specs=[anywhere, anywhere, vmem, vmem, vmem],
            out_specs=(vmem, vmem),
            scratch_shapes=[
                pltpu.VMEM((count, samples), jnp.bfloat16),
                pltpu.VMEM((samples, 2 * band), jnp.bfloat16),
                pltpu.VMEM((count, 2 * band), jnp.float32),
                pltpu.VMEM((1024, 128), jnp.float32),
                pltpu.VMEM((32, 2, 16, 128), jnp.bfloat16),
                pltpu.VMEM((32, 16, 128), jnp.bfloat16),
                pltpu.VMEM((SLOTS, 2, 16, 128), jnp.bfloat16),
                pltpu.VMEM((32, 2, 8, 128), jnp.bfloat16),
                pltpu.VMEM((320, 256), jnp.float32),
                pltpu.SemaphoreType.DMA((2 * CHUNKS,)),
                pltpu.SemaphoreType.DMA((COPIES,)),
                pltpu.SemaphoreType.DMA((COPIES,)),
            ],
            compiler_params=pltpu.CompilerParams(collective_id=0, has_side_effects=True),
        )(
            shot_traces,
            twiddles(samples, band),
            source_cell.reshape(4, 128),
            receiver_cell.reshape(4, 128),
            band_order.reshape(1, band),
        )
        return stack / jnp.maximum(counts, 1.0)[None, None, :, :]

    placed = (P(("band", "row"), None), P(("band", "row")), P(("band", "row")), P("band"))
    return jax.shard_map(
        local,
        mesh=mesh,
        in_specs=placed,
        out_specs=P(("band", "row"), None, None, None),
        check_vma=False,
    )
```

```python
import functools
import math

import jax
import jax.numpy as jnp
import numpy as np
from jax import lax
from jax.experimental import pallas as pl
from jax.experimental.pallas import tpu as pltpu
from jax.sharding import PartitionSpec as P

FLO = 64
SC = 128
RC = 128
MESH = pl.DeviceIdType.MESH
NT_DIMS = (((1,), (1,)), ((), ()))
CHUNKS = 4
REACH = 8


def twiddles(samples, band):
    bins = FLO + np.arange(band, dtype=np.int64)
    phase = (np.arange(samples, dtype=np.int64)[:, None] * bins[None, :]) % samples
    angle = (2.0 * math.pi * phase.astype(np.float32) / samples).astype(np.float32)
    scale = 1.0 / math.sqrt(samples)
    table = np.concatenate([np.cos(angle) * scale, -np.sin(angle) * scale], axis=1)
    return jnp.asarray(table.astype(np.float32)).astype(jnp.bfloat16)


FAR = 30
SELF = 31
TRANSIT = 32
SLOTS = TRANSIT + 16
FAR_TRANSIT = TRANSIT + 7
CHUNKED = ((14, 15), (12, 13), (10, 11), (9, 9))


def place_of(distance, side):
    return 2 * (distance - 1) + side


def transit_of(chunk, side):
    first, last = CHUNKED[chunk]
    return TRANSIT + 8 * side + (first - 9 if side == 0 else 15 - last)


def sources_of(chunk, side):
    first, last = CHUNKED[chunk]
    return first if side == 0 else 32 - last


ORDER = (
    ("chunk", 0),
    ("spread", 0),
    ("direct", 1),
    ("direct", 2),
    ("direct", 3),
    ("cells", 4),
    ("chunk", 1),
    ("direct", 8),
    ("cells", 8),
    ("chunk", 2),
    ("swap", 0),
    ("direct", 7),
    ("chunk", 3),
    ("swap", 4),
    ("bin", 1, 3),
    ("relay", 0),
    ("cells", 12),
    ("direct", 6),
    ("swap", 8),
    ("relay", 1),
    ("direct", 5),
    ("direct", 4),
    ("bin", 8, 8),
    ("swap", 12),
    ("relay", 2),
    ("bin", 7, 7),
    ("relay", 3),
    ("bin", 15, 16),
    ("bin", 13, 14),
    ("bin", 6, 6),
    ("bin", 11, 12),
    ("bin", 9, 10),
    ("bin", 4, 5),
)


def kernel(
    chips,
    traces_hbm,
    table_hbm,
    source_ref,
    receiver_ref,
    order_ref,
    stack_ref,
    counts_ref,
    traces,
    table,
    acc,
    staged,
    own,
    slots,
    cells,
    total,
    load_sem,
    send_sem,
    recv_sem,
):
    me = lax.axis_index("row")
    z = me // 2
    core = me % 2
    band = order_ref.shape[1]
    samples = traces.shape[1]
    part = samples // CHUNKS

    def peer(step, cross=0):
        return {"row": ((z + step + chips) % chips) * 2 + (core + cross) % 2}

    partner = peer(0, 1)
    towards = (1, -1)
    far_way = 1 - 2 * core

    loads = []
    for k in range(CHUNKS):
        span = pl.ds(k * part, part)
        loads.append(
            (
                pltpu.make_async_copy(table_hbm.at[span, :], table.at[span, :], load_sem.at[2 * k]),
                pltpu.make_async_copy(
                    traces_hbm.at[:, span], traces.at[:, span], load_sem.at[2 * k + 1]
                ),
            )
        )
    for pair in loads:
        for copy in pair:
            copy.start()

    barrier = pltpu.get_barrier_semaphore()
    greeted = [partner] + [
        peer(way * step, cross)
        for step in range(1, REACH + 1)
        for way in towards
        for cross in range(2)
    ]
    for who in greeted:
        pl.semaphore_signal(barrier, inc=1, device_id=who, device_id_type=MESH)

    source = source_ref[...]
    cells[SELF, 0, 0:4, :] = (source // 2).astype(jnp.float32).astype(jnp.bfloat16)
    cells[SELF, 0, 4:8, :] = (
        ((source % 2) * RC + receiver_ref[...]).astype(jnp.float32).astype(jnp.bfloat16)
    )
    total[...] = jnp.zeros_like(total)

    row = lax.broadcasted_iota(jnp.int32, (band, band), 0)
    col = lax.broadcasted_iota(jnp.int32, (band, band), 1)
    wanted = 4 * ((z + row % 32) % chips) + 2 * ((core + (row // 32) % 2) % 2) + row // 64
    place = (wanted == col).astype(jnp.float32).astype(jnp.bfloat16)
    holds = (row == jnp.broadcast_to(order_ref[...], (band, band))).astype(jnp.float32)
    pick = lax.dot_general(
        place, holds.astype(jnp.bfloat16), NT_DIMS, preferred_element_type=jnp.float32
    ).astype(jnp.bfloat16)

    for k in range(CHUNKS):
        span = pl.ds(k * part, part)
        for copy in loads[k]:
            copy.wait()
        piece = jnp.dot(traces[:, span], table[span, :], preferred_element_type=jnp.float32)
        if k == 0:
            acc[...] = piece
        else:
            acc[...] += piece
    for c in range(2):
        half = acc[:, c * band : (c + 1) * band].astype(jnp.bfloat16)
        turned = lax.dot_general(pick, half, NT_DIMS, preferred_element_type=jnp.float32)
        for f in range(2):
            for x in range(2):
                for b in range(4):
                    staged[pl.ds(x * 16 + b * 4 + c * 2 + f, 32, stride=32), :] = turned[
                        f * 64 + x * 32 : f * 64 + x * 32 + 32, b * 128 : (b + 1) * 128
                    ]
    own[...] = staged[...].reshape(32, 2, 16, 128).astype(jnp.bfloat16)
    slots[SELF, 0] = own[0, 0]

    pl.semaphore_wait(barrier, len(greeted))

    started = []

    def send(src, dst, who):
        n = len(started)
        copy = pltpu.make_async_remote_copy(
            src_ref=src,
            dst_ref=dst,
            send_sem=send_sem.at[n],
            recv_sem=recv_sem.at[n],
            device_id=who,
            device_id_type=MESH,
        )
        copy.start()
        started.append(copy)
        return copy

    def swap_cells(first, count):
        return send(cells.at[pl.ds(first, count), 0], cells.at[pl.ds(first, count), 1], partner)

    legs, spreads, swaps, arrivals, transits = {}, {}, {}, {}, {}

    def wait_all(copies):
        for copy in copies:
            copy.wait_recv()

    def cells_leg(distance, froms, hop):
        legs[distance] = [
            send(cells.at[froms[s], 0], cells.at[place_of(distance, s), 0], peer(hop * towards[s]))
            for s in range(2)
        ]

    def spread_cells(base):
        froms = (place_of(base, 0), place_of(base, 1)) if base else (SELF, SELF)
        spreads[base] = [
            send(
                cells.at[froms[s], 0],
                cells.at[place_of(base + step, s), 0],
                peer(towards[s] * step),
            )
            for step in (3, 2, 1)
            for s in range(2)
        ]

    def cells_onward(base):
        wait_all(legs[base])
        here = (place_of(base, 0), place_of(base, 1))
        if base == 8:
            cells_leg(12, here, 4)
            legs[16] = [send(cells.at[here[0] + core, 0], cells.at[FAR, 0], peer(8 * far_way))]
        spread_cells(base)
        swaps[base] = swap_cells(here[0], 2)

    def near_swap(base):
        wait_all(spreads[base])
        swap = swap_cells(place_of(base + 1, 0), 6)
        for step in (1, 2, 3):
            swaps[base + step] = swap
        if base == 12:
            wait_all(legs[16])
            swaps[16] = swap_cells(FAR, 1)

    def chunk(k):
        first, last = CHUNKED[k]
        size = last - first + 1
        if k == 0:
            transits["far"] = [send(own.at[16], slots.at[FAR_TRANSIT], peer(REACH * far_way))]
        transits[k] = [
            send(
                own.at[pl.ds(sources_of(k, s), size)],
                slots.at[pl.ds(transit_of(k, s), size)],
                peer(REACH * towards[s]),
            )
            for s in range(2)
        ]

    def direct(step):
        arrivals[step] = [
            send(
                own.at[step if s == 0 else 32 - step, cross],
                slots.at[place_of(step, s), cross],
                peer(towards[s] * step, cross),
            )
            for s in range(2)
            for cross in range(2)
        ]

    def relay(k):
        if k == 0:
            wait_all(transits["far"])
            arrivals[16] = [arrived_self] + [
                send(slots.at[FAR_TRANSIT, x], slots.at[FAR, x], peer(REACH * far_way, x))
                for x in range(2)
            ]
        wait_all(transits[k])
        first, last = CHUNKED[k]
        for distance in range(last, first - 1, -1):
            arrivals[distance] = [
                send(
                    slots.at[TRANSIT + 8 * s + (distance - 9 if s == 0 else 15 - distance), cross],
                    slots.at[place_of(distance, s), cross],
                    peer(towards[s] * (distance - REACH), cross),
                )
                for s in range(2)
                for cross in range(2)
            ]

    cells_leg(8, (SELF, SELF), 8)
    cells_leg(4, (SELF, SELF), 4)
    swap_self = swap_cells(SELF, 1)
    arrived_self = send(own.at[0, 1], slots.at[SELF, 1], partner)

    line = lax.broadcasted_iota(jnp.int32, (16, 128), 0).astype(jnp.float32)
    lines = [(line + 16.0 * g).astype(jnp.bfloat16) for g in range(4)]
    lane = lax.broadcasted_iota(jnp.int32, (16, 128), 1).astype(jnp.float32)
    lanes = [
        jnp.concatenate([(lane + 128.0 * g).astype(jnp.bfloat16)] * 8, axis=0) for g in range(2)
    ]
    one = jnp.ones((16, 128), jnp.bfloat16)
    none = jnp.zeros((16, 128), jnp.bfloat16)
    ones = jnp.ones((128, 128), jnp.bfloat16)
    nones = jnp.zeros((128, 128), jnp.bfloat16)

    def spread(rows, n, size=16):
        return jnp.broadcast_to(rows[n : n + 1, :], (size, 128)).astype(jnp.bfloat16)

    def binned(first, last):
        result = None
        for at in range(2 * first, 2 * last + 2):
            for cross in range(2):
                value = slots[at, cross].astype(jnp.float32)
                cell = cells[at, cross].astype(jnp.float32)
                for pair in range(2):
                    left, right = [], []
                    for b in (2 * pair, 2 * pair + 1):
                        high = spread(cell, b)
                        hit = [high == lines[g] for g in range(4)]
                        rows = []
                        for cf in range(4):
                            v = spread(value, b * 4 + cf)
                            rows += [jnp.where(h, v, none) for h in hit]
                        rows += [jnp.where(h, one, none) for h in hit]
                        left.append(jnp.concatenate(rows, axis=0))
                        low = spread(cell, 4 + b, 128).T
                        right.append(
                            jnp.concatenate(
                                [jnp.where(low == g, ones, nones) for g in lanes], axis=1
                            )
                        )
                    piece = jnp.dot(
                        jnp.concatenate(left, axis=1),
                        jnp.concatenate(right, axis=0),
                        preferred_element_type=jnp.float32,
                    )
                    result = piece if result is None else result + piece
        total[...] += result

    waited = []

    def bin_span(first, last):
        for distance in range(first, last + 1):
            wait_all(arrivals[distance])
            for swap in (swaps[distance], swap_self) if distance == 16 else (swaps[distance],):
                if not any(swap is other for other in waited):
                    waited.append(swap)
                    swap.wait_recv()
        binned(first - 1, last - 1)

    steps = {
        "chunk": chunk,
        "direct": direct,
        "relay": relay,
        "spread": spread_cells,
        "cells": cells_onward,
        "swap": near_swap,
        "bin": bin_span,
    }
    for what, *given in ORDER:
        steps[what](*given)

    for cf in range(4):
        for odd in range(2):
            stack_ref[cf % 2, cf // 2, pl.ds(odd, 64, stride=2), :] = total[
                cf * 64 : cf * 64 + 64, odd * 128 : odd * 128 + 128
            ]
    for odd in range(2):
        counts_ref[pl.ds(odd, 64, stride=2), :] = jnp.maximum(
            total[256:320, odd * 128 : odd * 128 + 128], 1.0
        )
    for copy in started:
        copy.wait_send()


COPIES = 140


def solution(mesh):
    rows = mesh.shape["row"]

    def local(shot_traces, source_cell, receiver_cell, band_order):
        count, samples = shot_traces.shape
        band = band_order.shape[0]
        per = band // rows
        vmem = pl.BlockSpec(memory_space=pltpu.VMEM)
        anywhere = pl.BlockSpec(memory_space=pltpu.HBM)
        stack, counts = pl.pallas_call(
            functools.partial(kernel, rows // 2),
            out_shape=(
                jax.ShapeDtypeStruct((per, 2, SC, RC), jnp.float32),
                jax.ShapeDtypeStruct((SC, RC), jnp.float32),
            ),
            in_specs=[anywhere, anywhere, vmem, vmem, vmem],
            out_specs=(vmem, vmem),
            scratch_shapes=[
                pltpu.VMEM((count, samples), jnp.bfloat16),
                pltpu.VMEM((samples, 2 * band), jnp.bfloat16),
                pltpu.VMEM((count, 2 * band), jnp.float32),
                pltpu.VMEM((1024, 128), jnp.float32),
                pltpu.VMEM((32, 2, 16, 128), jnp.bfloat16),
                pltpu.VMEM((SLOTS, 2, 16, 128), jnp.bfloat16),
                pltpu.VMEM((32, 2, 8, 128), jnp.bfloat16),
                pltpu.VMEM((320, 256), jnp.float32),
                pltpu.SemaphoreType.DMA((2 * CHUNKS,)),
                pltpu.SemaphoreType.DMA((COPIES,)),
                pltpu.SemaphoreType.DMA((COPIES,)),
            ],
            compiler_params=pltpu.CompilerParams(
                collective_id=0, has_side_effects=True, vmem_limit_bytes=55_000_000
            ),
        )(
            shot_traces,
            twiddles(samples, band),
            source_cell.reshape(4, 128),
            receiver_cell.reshape(4, 128),
            band_order.reshape(1, band),
        )
        return stack / counts[None, None, :, :]

    placed = (P(("band", "row"), None), P(("band", "row")), P(("band", "row")), P("band"))
    return jax.shard_map(
        local,
        mesh=mesh,
        in_specs=placed,
        out_specs=P(("band", "row"), None, None, None),
        check_vma=False,
    )
```

```python
import functools
import math

import jax
import jax.numpy as jnp
import numpy as np
from jax import lax
from jax.experimental import pallas as pl
from jax.experimental.pallas import tpu as pltpu
from jax.sharding import PartitionSpec as P

FLO = 64
SC = 128
RC = 128
MESH = pl.DeviceIdType.MESH
NT_DIMS = (((1,), (1,)), ((), ()))
CHUNKS = 4
REACH = 8


def twiddles(samples, band):
    bins = FLO + np.arange(band, dtype=np.int64)
    phase = (np.arange(samples, dtype=np.int64)[:, None] * bins[None, :]) % samples
    angle = (2.0 * math.pi * phase.astype(np.float32) / samples).astype(np.float32)
    scale = 1.0 / math.sqrt(samples)
    table = np.concatenate([np.cos(angle) * scale, -np.sin(angle) * scale], axis=1)
    return jnp.asarray(table.astype(np.float32)).astype(jnp.bfloat16)


FAR = 30
SELF = 31
TRANSIT = 32
SLOTS = TRANSIT + 16
FAR_TRANSIT = TRANSIT + 7
CHUNKED = ((14, 15), (12, 13), (10, 11), (9, 9))


def place_of(distance, side):
    return 2 * (distance - 1) + side


def transit_of(chunk, side):
    first, last = CHUNKED[chunk]
    return TRANSIT + 8 * side + (first - 9 if side == 0 else 15 - last)


def sources_of(chunk, side):
    first, last = CHUNKED[chunk]
    return first if side == 0 else 32 - last


ORDER = (
    ("chunk", 0),
    ("spread", 0),
    ("direct", 1),
    ("direct", 2),
    ("direct", 3),
    ("cells", 4),
    ("chunk", 1),
    ("direct", 8),
    ("cells", 8),
    ("chunk", 2),
    ("swap", 0),
    ("direct", 7),
    ("chunk", 3),
    ("swap", 4),
    ("bin", 1, 3),
    ("relay", 0),
    ("cells", 12),
    ("direct", 6),
    ("swap", 8),
    ("relay", 1),
    ("direct", 5),
    ("direct", 4),
    ("bin", 8, 8),
    ("swap", 12),
    ("relay", 2),
    ("bin", 7, 7),
    ("relay", 3),
    ("bin", 15, 16),
    ("bin", 13, 14),
    ("bin", 6, 6),
    ("bin", 11, 12),
    ("bin", 9, 10),
    ("bin", 4, 5),
)


def kernel(
    chips,
    traces_hbm,
    table_hbm,
    source_hbm,
    receiver_hbm,
    order_hbm,
    stack_ref,
    counts_ref,
    traces,
    table,
    source_ref,
    receiver_ref,
    order_ref,
    acc,
    staged,
    own,
    slots,
    cells,
    total,
    load_sem,
    send_sem,
    recv_sem,
):
    me = lax.axis_index("row")
    z = me // 2
    core = me % 2
    band = order_ref.shape[1]
    samples = traces.shape[1]
    part = samples // CHUNKS

    def peer(step, cross=0):
        return {"row": ((z + step + chips) % chips) * 2 + (core + cross) % 2}

    partner = peer(0, 1)
    towards = (1, -1)
    far_way = 1 - 2 * core

    barrier = pltpu.get_barrier_semaphore()
    greeted = [partner] + [
        peer(way * step, cross)
        for step in range(REACH, 0, -1)
        for way in towards
        for cross in range(2)
    ]
    for who in greeted:
        pl.semaphore_signal(barrier, inc=1, device_id=who, device_id_type=MESH)

    small = [
        pltpu.make_async_copy(src, dst, load_sem.at[2 * CHUNKS + n])
        for n, (src, dst) in enumerate(
            ((source_hbm, source_ref), (receiver_hbm, receiver_ref), (order_hbm, order_ref))
        )
    ]
    for copy in small:
        copy.start()
    loads = []
    for k in range(CHUNKS):
        span = pl.ds(k * part, part)
        loads.append(
            (
                pltpu.make_async_copy(table_hbm.at[span, :], table.at[span, :], load_sem.at[2 * k]),
                pltpu.make_async_copy(
                    traces_hbm.at[:, span], traces.at[:, span], load_sem.at[2 * k + 1]
                ),
            )
        )
    for pair in loads:
        for copy in pair:
            copy.start()

    for copy in small:
        copy.wait()
    source = source_ref[...]
    cells[SELF, 0, 0:4, :] = (source // 2).astype(jnp.float32).astype(jnp.bfloat16)
    cells[SELF, 0, 4:8, :] = (
        ((source % 2) * RC + receiver_ref[...]).astype(jnp.float32).astype(jnp.bfloat16)
    )
    total[...] = jnp.zeros_like(total)

    row = lax.broadcasted_iota(jnp.int32, (band, band), 0)
    col = lax.broadcasted_iota(jnp.int32, (band, band), 1)
    wanted = 4 * ((z + row % 32) % chips) + 2 * ((core + (row // 32) % 2) % 2) + row // 64
    place = (wanted == col).astype(jnp.float32).astype(jnp.bfloat16)
    holds = (row == jnp.broadcast_to(order_ref[...], (band, band))).astype(jnp.float32)
    pick = lax.dot_general(
        place, holds.astype(jnp.bfloat16), NT_DIMS, preferred_element_type=jnp.float32
    ).astype(jnp.bfloat16)

    for k in range(CHUNKS):
        span = pl.ds(k * part, part)
        for copy in loads[k]:
            copy.wait()
        piece = jnp.dot(traces[:, span], table[span, :], preferred_element_type=jnp.float32)
        if k == 0:
            acc[...] = piece
        else:
            acc[...] += piece
    for c in range(2):
        half = acc[:, c * band : (c + 1) * band].astype(jnp.bfloat16)
        turned = lax.dot_general(pick, half, NT_DIMS, preferred_element_type=jnp.float32)
        for f in range(2):
            for x in range(2):
                for b in range(4):
                    staged[pl.ds(x * 16 + b * 4 + c * 2 + f, 32, stride=32), :] = turned[
                        f * 64 + x * 32 : f * 64 + x * 32 + 32, b * 128 : (b + 1) * 128
                    ]
    own[...] = staged[...].reshape(32, 2, 16, 128).astype(jnp.bfloat16)
    slots[SELF, 0] = own[0, 0]

    pl.semaphore_wait(barrier, len(greeted))

    started = []

    def send(src, dst, who):
        n = len(started)
        copy = pltpu.make_async_remote_copy(
            src_ref=src,
            dst_ref=dst,
            send_sem=send_sem.at[n],
            recv_sem=recv_sem.at[n],
            device_id=who,
            device_id_type=MESH,
        )
        copy.start()
        started.append(copy)
        return copy

    def swap_cells(first, count):
        return send(cells.at[pl.ds(first, count), 0], cells.at[pl.ds(first, count), 1], partner)

    legs, spreads, swaps, arrivals, transits = {}, {}, {}, {}, {}

    def wait_all(copies):
        for copy in copies:
            copy.wait_recv()

    def cells_leg(distance, froms, hop):
        legs[distance] = [
            send(cells.at[froms[s], 0], cells.at[place_of(distance, s), 0], peer(hop * towards[s]))
            for s in range(2)
        ]

    def spread_cells(base):
        froms = (place_of(base, 0), place_of(base, 1)) if base else (SELF, SELF)
        spreads[base] = [
            send(
                cells.at[froms[s], 0],
                cells.at[place_of(base + step, s), 0],
                peer(towards[s] * step),
            )
            for step in (3, 2, 1)
            for s in range(2)
        ]

    def cells_onward(base):
        wait_all(legs[base])
        here = (place_of(base, 0), place_of(base, 1))
        if base == 8:
            cells_leg(12, here, 4)
            legs[16] = [send(cells.at[here[0] + core, 0], cells.at[FAR, 0], peer(8 * far_way))]
        spread_cells(base)
        swaps[base] = swap_cells(here[0], 2)

    def near_swap(base):
        wait_all(spreads[base])
        swap = swap_cells(place_of(base + 1, 0), 6)
        for step in (1, 2, 3):
            swaps[base + step] = swap
        if base == 12:
            wait_all(legs[16])
            swaps[16] = swap_cells(FAR, 1)

    def chunk(k):
        first, last = CHUNKED[k]
        size = last - first + 1
        if k == 0:
            transits["far"] = [send(own.at[16], slots.at[FAR_TRANSIT], peer(REACH * far_way))]
        transits[k] = [
            send(
                own.at[pl.ds(sources_of(k, s), size)],
                slots.at[pl.ds(transit_of(k, s), size)],
                peer(REACH * towards[s]),
            )
            for s in range(2)
        ]

    def direct(step):
        arrivals[step] = [
            send(
                own.at[step if s == 0 else 32 - step, cross],
                slots.at[place_of(step, s), cross],
                peer(towards[s] * step, cross),
            )
            for s in range(2)
            for cross in range(2)
        ]

    def relay(k):
        if k == 0:
            wait_all(transits["far"])
            arrivals[16] = [arrived_self] + [
                send(slots.at[FAR_TRANSIT, x], slots.at[FAR, x], peer(REACH * far_way, x))
                for x in range(2)
            ]
        wait_all(transits[k])
        first, last = CHUNKED[k]
        for distance in range(last, first - 1, -1):
            arrivals[distance] = [
                send(
                    slots.at[TRANSIT + 8 * s + (distance - 9 if s == 0 else 15 - distance), cross],
                    slots.at[place_of(distance, s), cross],
                    peer(towards[s] * (distance - REACH), cross),
                )
                for s in range(2)
                for cross in range(2)
            ]

    cells_leg(8, (SELF, SELF), 8)
    cells_leg(4, (SELF, SELF), 4)
    swap_self = swap_cells(SELF, 1)
    arrived_self = send(own.at[0, 1], slots.at[SELF, 1], partner)

    line = lax.broadcasted_iota(jnp.int32, (16, 128), 0).astype(jnp.float32)
    lines = [(line + 16.0 * g).astype(jnp.bfloat16) for g in range(4)]
    lane = lax.broadcasted_iota(jnp.int32, (16, 128), 1).astype(jnp.float32)
    lanes = [
        jnp.concatenate([(lane + 128.0 * g).astype(jnp.bfloat16)] * 8, axis=0) for g in range(2)
    ]
    one = jnp.ones((16, 128), jnp.bfloat16)
    none = jnp.zeros((16, 128), jnp.bfloat16)
    ones = jnp.ones((128, 128), jnp.bfloat16)
    nones = jnp.zeros((128, 128), jnp.bfloat16)

    def spread(rows, n, size=16):
        return jnp.broadcast_to(rows[n : n + 1, :], (size, 128)).astype(jnp.bfloat16)

    def binned(first, last):
        result = None
        for at in range(2 * first, 2 * last + 2):
            for cross in range(2):
                value = slots[at, cross].astype(jnp.float32)
                cell = cells[at, cross].astype(jnp.float32)
                for pair in range(2):
                    left, right = [], []
                    for b in (2 * pair, 2 * pair + 1):
                        high = spread(cell, b)
                        hit = [high == lines[g] for g in range(4)]
                        rows = []
                        for cf in range(4):
                            v = spread(value, b * 4 + cf)
                            rows += [jnp.where(h, v, none) for h in hit]
                        rows += [jnp.where(h, one, none) for h in hit]
                        left.append(jnp.concatenate(rows, axis=0))
                        low = spread(cell, 4 + b, 128).T
                        right.append(
                            jnp.concatenate(
                                [jnp.where(low == g, ones, nones) for g in lanes], axis=1
                            )
                        )
                    piece = jnp.dot(
                        jnp.concatenate(left, axis=1),
                        jnp.concatenate(right, axis=0),
                        preferred_element_type=jnp.float32,
                    )
                    result = piece if result is None else result + piece
        total[...] += result

    waited = []

    def bin_span(first, last):
        for distance in range(first, last + 1):
            wait_all(arrivals[distance])
            for swap in (swaps[distance], swap_self) if distance == 16 else (swaps[distance],):
                if not any(swap is other for other in waited):
                    waited.append(swap)
                    swap.wait_recv()
        binned(first - 1, last - 1)

    steps = {
        "chunk": chunk,
        "direct": direct,
        "relay": relay,
        "spread": spread_cells,
        "cells": cells_onward,
        "swap": near_swap,
        "bin": bin_span,
    }
    for what, *given in ORDER:
        steps[what](*given)

    for cf in range(4):
        for odd in range(2):
            stack_ref[cf % 2, cf // 2, pl.ds(odd, 64, stride=2), :] = total[
                cf * 64 : cf * 64 + 64, odd * 128 : odd * 128 + 128
            ]
    for odd in range(2):
        counts_ref[pl.ds(odd, 64, stride=2), :] = jnp.maximum(
            total[256:320, odd * 128 : odd * 128 + 128], 1.0
        )
    for copy in started:
        copy.wait_send()


COPIES = 140


def solution(mesh):
    rows = mesh.shape["row"]

    def local(shot_traces, source_cell, receiver_cell, band_order):
        count, samples = shot_traces.shape
        band = band_order.shape[0]
        per = band // rows
        vmem = pl.BlockSpec(memory_space=pltpu.VMEM)
        anywhere = pl.BlockSpec(memory_space=pl.ANY)
        stack, counts = pl.pallas_call(
            functools.partial(kernel, rows // 2),
            out_shape=(
                jax.ShapeDtypeStruct((per, 2, SC, RC), jnp.float32),
                jax.ShapeDtypeStruct((SC, RC), jnp.float32),
            ),
            in_specs=[anywhere] * 5,
            out_specs=(vmem, vmem),
            scratch_shapes=[
                pltpu.VMEM((count, samples), jnp.bfloat16),
                pltpu.VMEM((samples, 2 * band), jnp.bfloat16),
                pltpu.VMEM((4, 128), jnp.int32),
                pltpu.VMEM((4, 128), jnp.int32),
                pltpu.VMEM((1, band), jnp.int32),
                pltpu.VMEM((count, 2 * band), jnp.float32),
                pltpu.VMEM((1024, 128), jnp.float32),
                pltpu.VMEM((32, 2, 16, 128), jnp.bfloat16),
                pltpu.VMEM((SLOTS, 2, 16, 128), jnp.bfloat16),
                pltpu.VMEM((32, 2, 8, 128), jnp.bfloat16),
                pltpu.VMEM((320, 256), jnp.float32),
                pltpu.SemaphoreType.DMA((2 * CHUNKS + 3,)),
                pltpu.SemaphoreType.DMA((COPIES,)),
                pltpu.SemaphoreType.DMA((COPIES,)),
            ],
            compiler_params=pltpu.CompilerParams(
                collective_id=0, has_side_effects=True, vmem_limit_bytes=55_000_000
            ),
        )(
            shot_traces,
            twiddles(samples, band),
            pltpu.with_memory_space_constraint(source_cell.reshape(4, 128), pltpu.HBM),
            pltpu.with_memory_space_constraint(receiver_cell.reshape(4, 128), pltpu.HBM),
            pltpu.with_memory_space_constraint(band_order.reshape(1, band), pltpu.HBM),
        )
        return stack / counts[None, None, :, :]

    placed = (P(("band", "row"), None), P(("band", "row")), P(("band", "row")), P("band"))
    return jax.shard_map(
        local,
        mesh=mesh,
        in_specs=placed,
        out_specs=P(("band", "row"), None, None, None),
        check_vma=False,
    )
```
